512 devices in a mesh: feat: 64 (over y, z), samp: 8 (over x, core).
Axes of the slice: x: 4, y: 4, z: 16, core: 2. Of those that a mesh axis runs over, the one named last changes fastest.
Arguments:
- features: bfloat16 [1024, 524288], P('samp', 'feat'), may hold values from -14 to 14
- labels: int32 [1024, 32], P('samp'), may hold values from -1 to 1, as said below
- alpha_start: float32 [1024, 32], P('samp'), may hold values from 0 to 1
- order: int32 [2, 1024], P(None, 'samp'), may hold values from 0 to 127, as said below
Outputs:
- alpha: float32 [1024, 32], P('samp')
- scores: float32 [1024, 32], P('samp')
The draws below stay inside these ranges and needn't reach their ends.
Inputs may be any that keep to these rules, and one draw needn't show every extreme that they name: `labels`: every entry is -1 or +1. `order`: for each round, each aligned block of 128 entries (one partition) is a permutation of 0 to 127.
All inputs are finite; a program needn't handle non-finite values.
Results may differ from the reference program's by a relative error of at most 0.004.
Values may be sent and summed in bfloat16 or wider, within the bound.
A program may use at most 64 MiB of HBM per device.

```python
import math
import jax
import jax.numpy as jnp
from jax import lax

FEAT_DEV = 8192
LABELS = 32
ROWS_DEV = 128
BLOCK = 64
ROUNDS = 2
FEATURES = 524288
ROWS = 1024


def draw_features(key, part):
    key_values, key_scale, key_common, key_coef = jax.random.split(jax.random.fold_in(key, 11), 4)
    group_width = FEAT_DEV // 2
    group_count = FEATURES // group_width
    log_scale = jax.random.uniform(key_scale, (group_count,), jnp.float32, math.log(0.35), math.log(2.8))
    column_scale = jnp.repeat(jnp.exp(log_scale), group_width)
    raw_values = jnp.clip(jax.random.normal(key_values, (ROWS, FEATURES), jnp.float32), -5.0, 5.0)
    return (raw_values * column_scale[None, :]).astype(jnp.bfloat16)


def draw_labels(key, part):
    coins = jax.random.randint(jax.random.fold_in(key, 23), (ROWS, LABELS), 0, 2, dtype=jnp.int32)
    return (2 * coins - 1).astype(jnp.int32)


def draw_order(key, part):
    part_total = ROWS // ROWS_DEV
    subkeys = jax.random.split(jax.random.fold_in(key, 37), ROUNDS * part_total)
    perms = jax.vmap(lambda subkey: jax.random.permutation(subkey, ROWS_DEV))(subkeys)
    return perms.reshape(ROUNDS, ROWS).astype(jnp.int32)


def levels(own_key, shape, cuts, low, high):
    loudness, own = 1.0, jax.random.fold_in(own_key, 6)
    for dim, blocks in cuts:
        heights = jnp.exp(jax.random.uniform(jax.random.fold_in(own, dim), (blocks,), jnp.float32, low / len(cuts), high / len(cuts)))
        loudness = loudness * jnp.repeat(heights, shape[dim] // blocks).reshape([-1 if axis == dim else 1 for axis in range(len(shape))])
    return loudness


def setup_inputs(seed: int = 0) -> dict:
    streams_of = jax.random.split(jax.random.key(seed), 5)
    features = draw_features(jax.random.fold_in(streams_of[4], 71), 0)
    labels = draw_labels(jax.random.fold_in(streams_of[4], 71), 0)
    alpha_start = jnp.clip(1.0 * jax.random.uniform(streams_of[2], (ROWS, LABELS), jnp.float32) ** levels(streams_of[2], (ROWS, LABELS), ((0, 8),), -0.2, 0.2), 0.0, 1.0)
    order = draw_order(jax.random.fold_in(streams_of[4], 71), 0)
    return dict(features=features, labels=labels, alpha_start=alpha_start, order=order)


reg_scale = 0.9


def part_slice(source, part_index):
    return lax.dynamic_slice_in_dim(source, part_index * ROWS_DEV, ROWS_DEV, 0)


def contract_rows(left_side, right_side):
    return lax.dot_general(left_side, right_side, (((0,), (0,)), ((), ())), preferred_element_type=jnp.float32)


def contract_cols(left_side, right_side):
    return lax.dot_general(left_side, right_side, (((1,), (1,)), ((), ())), preferred_element_type=jnp.float32)


def local_round(weights, part_rows, part_signs, part_alpha, part_norms, row_order, lam_total):
    local_weights = weights
    local_alpha = part_alpha
    for block_num in range(ROWS_DEV // BLOCK):
        chosen = row_order[block_num * BLOCK:(block_num + 1) * BLOCK]
        picked = jnp.take(part_rows, chosen, axis=0)
        margins = contract_cols(picked, local_weights.astype(jnp.bfloat16))
        before = jnp.take(local_alpha, chosen, axis=0)
        block_signs = jnp.take(part_signs, chosen, axis=0)
        block_norms = jnp.take(part_norms, chosen, axis=0)
        updated = jnp.clip(before + lam_total * (1.0 - block_signs * margins) / block_norms[:, None], 0.0, 1.0)
        change = ((updated - before) * block_signs).astype(jnp.bfloat16)
        local_alpha = local_alpha.at[chosen].set(updated)
        local_weights = local_weights + contract_rows(change, picked) / lam_total
    return local_weights, local_alpha


def reference(features, labels, alpha_start, order):
    part_count = ROWS // ROWS_DEV
    lam_total = reg_scale * FEATURES
    signs_all = labels.astype(jnp.float32)
    part_ids = jnp.arange(part_count, dtype=jnp.int32)

    def row_norms(part_index):
        part_rows = part_slice(features, part_index)
        return jnp.einsum("rf,rf->r", part_rows, part_rows, preferred_element_type=jnp.float32) + 1.0

    norms_all = lax.map(row_norms, part_ids)

    def warm_part(running, part_index):
        part_rows = part_slice(features, part_index)
        coeffs = (part_slice(alpha_start, part_index) * part_slice(signs_all, part_index)).astype(jnp.bfloat16)
        piece = lax.optimization_barrier((contract_rows(coeffs, part_rows) / lam_total).astype(jnp.bfloat16))
        return running + piece.astype(jnp.float32), None

    weights, _ = lax.scan(warm_part, jnp.zeros((LABELS, FEATURES), jnp.float32), part_ids)
    alpha_now = alpha_start
    for round_num in range(ROUNDS):
        def round_part(running, part_index, weights=weights, alpha_now=alpha_now, round_num=round_num):
            part_alpha = part_slice(alpha_now, part_index)
            row_order = lax.dynamic_slice_in_dim(order[round_num], part_index * ROWS_DEV, ROWS_DEV, 0)
            local_weights, local_alpha = local_round(weights, part_slice(features, part_index), part_slice(signs_all, part_index), part_alpha, norms_all[part_index], row_order, lam_total)
            delta_weights = lax.optimization_barrier((local_weights - weights).astype(jnp.bfloat16))
            return running + delta_weights.astype(jnp.float32), part_alpha + (local_alpha - part_alpha) / part_count

        summed, alpha_parts = lax.scan(round_part, jnp.zeros((LABELS, FEATURES), jnp.float32), part_ids)
        weights = weights + summed / part_count
        alpha_now = alpha_parts.reshape(ROWS, LABELS)
    weights_half = weights.astype(jnp.bfloat16)

    def score_part(part_index):
        return contract_cols(part_slice(features, part_index), weights_half)

    scores = lax.map(score_part, part_ids).reshape(ROWS, LABELS)
    return alpha_now, scores
```

```python
import functools

import jax
import jax.numpy as jnp
from jax import lax
from jax.experimental import pallas as pl
from jax.experimental.pallas import tpu as pltpu
from jax.sharding import Mesh
from jax.sharding import PartitionSpec as P

BLOCK = 64
ROUNDS = 2
GRID = (4, 16, 4, 2)
NAMES = ("y", "z", "x", "c")
MESH = pl.DeviceIdType.MESH
FEAT = ("y", "z")
SAMP = ("x", "c")

reg_scale = 0.9


def mm(left, right):
    return lax.dot_general(left, right, (((1,), (0,)), ((), ())), preferred_element_type=jnp.float32)


def mm_t(left, right):
    return lax.dot_general(left, right, (((1,), (1,)), ((), ())), preferred_element_type=jnp.float32)


def kernel(
    sizes,
    lam_total,
    feat_hbm,
    labels_ref,
    alpha_ref,
    order_ref,
    alpha_out,
    scores_out,
    own,
    turned,
    coef,
    wacc,
    part_m,
    got_m,
    got_z,
    signs_s,
    alpha_s,
    last,
    gram_p,
    gram_y,
    gram_z,
    gram,
    loc_sem,
    turn_send,
    turn_recv,
    coef_send,
    coef_recv,
    m_send,
    m_recv,
    z_send,
    z_recv,
    g_send,
    g_recv,
    last_send,
    last_recv,
):
    ny, nz, nx, nc = sizes
    y, z, x, c = (lax.axis_index(name) for name in NAMES)
    ns = nx * nc
    samp = x * nc + c
    rows, cols = feat_hbm.shape
    lab = labels_ref.shape[1]
    lp = lab // ny
    gp = rows // ny
    share = cols // ns
    pieces = ny * ns
    me = y * ns + samp

    def samp_dev(peer):
        return (y, z, peer // nc, peer % nc)

    def plane_dev(peer):
        peer_s = peer % ns
        return (peer // ns, z, peer_s // nc, peer_s % nc)

    def z_dev(peer):
        return (y, peer, x, c)

    def y_dev(peer):
        return (peer, z, x, c)

    def others(count, index, body):
        def step(i, carry):
            body(lax.rem(index + i, count))
            return carry

        lax.fori_loop(1, count, step, 0)

    def send(src, dst, s_sem, r_sem, dev):
        pltpu.make_async_remote_copy(
            src_ref=src, dst_ref=dst, send_sem=s_sem, recv_sem=r_sem, device_id=dev, device_id_type=MESH
        ).start()

    def wait_bytes(ref, sem):
        pltpu.make_async_copy(ref, ref, sem).wait()

    def tile(ref, peer_s, peer_y):
        return ref.at[pl.ds(pl.multiple_of(peer_y * lp, lp), lp), pl.ds(pl.multiple_of(peer_s * rows, rows), rows)]

    barrier = pltpu.get_barrier_semaphore()

    def hello(dev):
        pl.semaphore_signal(barrier, inc=1, device_id=dev, device_id_type=MESH)

    others(pieces, me, lambda p: hello(plane_dev(p)))
    others(nz, z, lambda p: hello(z_dev(p)))

    load_own = pltpu.make_async_copy(feat_hbm, own, loc_sem.at[0])
    load_own.start()
    my_rows = pl.ds(pl.multiple_of(samp * rows, rows), rows)
    load_turn = pltpu.make_async_copy(
        feat_hbm.at[:, pl.ds(pl.multiple_of(samp * share, share), share)], turned.at[my_rows], loc_sem.at[1]
    )
    load_turn.start()

    signs_s[...] = labels_ref[...].astype(jnp.float32).T
    alpha_s[...] = alpha_ref[...].T
    coef[0, :, my_rows] = (alpha_s[...] * signs_s[...]).astype(jnp.bfloat16).astype(jnp.float32)

    pl.semaphore_wait(barrier, pieces - 1 + nz - 1)

    others(
        ns,
        samp,
        lambda p: send(
            coef.at[0, :, my_rows], coef.at[0, :, my_rows], coef_send.at[0], coef_recv.at[0], samp_dev(p)
        ),
    )
    others(
        ns,
        samp,
        lambda p: send(
            feat_hbm.at[:, pl.ds(pl.multiple_of(p * share, share), share)],
            turned.at[my_rows],
            turn_send,
            turn_recv,
            samp_dev(p),
        ),
    )

    load_own.wait()
    gram_p[...] = mm_t(own[...], own[...])

    def gpiece(ref, peer_y):
        return ref.at[pl.ds(pl.multiple_of(peer_y * gp, gp), gp)]

    others(ny, y, lambda p: send(gpiece(gram_p, p), gram_y.at[y], g_send.at[0], g_recv.at[0], y_dev(p)))
    gram_y[y] = gpiece(gram_p, y)[...]
    if ny > 1:
        wait_bytes(gram_y.at[pl.ds(0, ny - 1)], g_recv.at[0])
    gram_z[z] = jnp.sum(gram_y[...], axis=0)
    others(nz, z, lambda p: send(gram_z.at[z], gram_z.at[z], g_send.at[1], g_recv.at[1], z_dev(p)))
    wait_bytes(gram_z.at[pl.ds(0, nz - 1)], g_recv.at[1])
    gpiece(gram, y)[...] = jnp.sum(gram_z[...], axis=0)
    others(ny, y, lambda p: send(gpiece(gram, y), gpiece(gram, y), g_send.at[2], g_recv.at[2], y_dev(p)))
    if ny > 1:
        wait_bytes(gram.at[pl.ds(0, rows - gp)], g_recv.at[2])

    g_all = gram[...]
    g_high = g_all.astype(jnp.bfloat16)
    g_low = (g_all - g_high.astype(jnp.float32)).astype(jnp.bfloat16)
    row_i = lax.broadcasted_iota(jnp.int32, (rows, rows), 0)
    col_i = lax.broadcasted_iota(jnp.int32, (rows, rows), 1)
    norms = 1.0 + jnp.sum(jnp.where(row_i == col_i, g_all, 0.0), axis=0, keepdims=True)
    early = (lax.broadcasted_iota(jnp.int32, (8, rows), 1) < BLOCK).astype(jnp.bfloat16)
    firsts = []
    for r in range(ROUNDS):
        hot = (row_i == order_ref[r : r + 1, :]).astype(jnp.bfloat16)
        firsts.append(mm_t(early, hot)[0:1] > 0.5)

    my_labels = pl.ds(pl.multiple_of(y * lp, lp), lp)
    sign = signs_s[my_labels, :]
    alpha = alpha_s[my_labels, :]

    load_turn.wait()
    wait_bytes(coef.at[0, :, pl.ds(0, (ns - 1) * rows)], coef_recv.at[0])
    wait_bytes(turned.at[pl.ds(0, (ns - 1) * rows)], turn_recv)

    for r in range(ROUNDS + 1):
        step = mm(coef[r].astype(jnp.bfloat16), turned[...])
        wacc[...] = step if r == 0 else wacc[...] + step * (1.0 / ns)
        part_m[r] = mm_t((wacc[...] * (1.0 / lam_total)).astype(jnp.bfloat16), turned[...])
        got_m[r, me] = tile(part_m.at[r], samp, y)[...]
        others(
            pieces,
            me,
            lambda p: send(tile(part_m.at[r], p % ns, p // ns), got_m.at[r, me], m_send.at[r], m_recv.at[r], plane_dev(p)),
        )
        wait_bytes(got_m.at[r, pl.ds(0, pieces - 1)], m_recv.at[r])
        got_z[r, z] = jnp.sum(got_m[r], axis=0)
        others(nz, z, lambda p: send(got_z.at[r, z], got_z.at[r, z], z_send.at[r], z_recv.at[r], z_dev(p)))
        wait_bytes(got_z.at[r, pl.ds(0, nz - 1)], z_recv.at[r])
        margins = jnp.sum(got_z[r], axis=0)
        if r == ROUNDS:
            break
        first = firsts[r]
        up_0 = jnp.clip(alpha + lam_total * (1.0 - sign * margins) / norms, 0.0, 1.0)
        ch_0 = jnp.where(first, (up_0 - alpha) * sign, 0.0).astype(jnp.bfloat16)
        moved = mm(ch_0, g_high) + mm(ch_0, g_low)
        margins = margins + moved * (1.0 / lam_total)
        up_1 = jnp.clip(alpha + lam_total * (1.0 - sign * margins) / norms, 0.0, 1.0)
        ch_1 = ((up_1 - alpha) * sign).astype(jnp.bfloat16)
        change = jnp.where(first, ch_0.astype(jnp.float32), ch_1.astype(jnp.float32))
        alpha = alpha + (jnp.where(first, up_0, up_1) - alpha) * (1.0 / ns)
        spot = tile(coef.at[r + 1], samp, y)
        spot[...] = change
        others(
            pieces,
            me,
            lambda p: send(spot, spot, coef_send.at[r + 1], coef_recv.at[r + 1], plane_dev(p)),
        )
        if r == ROUNDS - 1:
            last[0, my_labels] = alpha
            others(
                ny,
                y,
                lambda p: send(last.at[0, my_labels], last.at[0, my_labels], last_send.at[0], last_recv.at[0], y_dev(p)),
            )
        wait_bytes(got_m.at[r + 1, pl.ds(0, pieces - 1)], coef_recv.at[r + 1])

    last[1, my_labels] = margins
    others(
        ny, y, lambda p: send(last.at[1, my_labels], last.at[1, my_labels], last_send.at[1], last_recv.at[1], y_dev(p))
    )
    if ny > 1:
        wait_bytes(last.at[0, pl.ds(0, lab - lp)], last_recv.at[0])
    alpha_out[...] = last[0].T
    if ny > 1:
        wait_bytes(last.at[1, pl.ds(0, lab - lp)], last_recv.at[1])
    scores_out[...] = last[1].T

    wait_bytes(turned.at[pl.ds(0, (ns - 1) * rows)], turn_send)
    wait_bytes(coef.at[0, :, pl.ds(0, (ns - 1) * rows)], coef_send.at[0])
    for r in range(ROUNDS + 1):
        wait_bytes(got_m.at[r, pl.ds(0, pieces - 1)], m_send.at[r])
        wait_bytes(got_z.at[r, pl.ds(0, nz - 1)], z_send.at[r])
        if r:
            wait_bytes(got_m.at[r, pl.ds(0, pieces - 1)], coef_send.at[r])
    wait_bytes(gram_z.at[pl.ds(0, nz - 1)], g_send.at[1])
    if ny > 1:
        wait_bytes(gram_y.at[pl.ds(0, ny - 1)], g_send.at[0])
        wait_bytes(gram_y.at[pl.ds(0, ny - 1)], g_send.at[2])
        for i in range(2):
            wait_bytes(last.at[i, pl.ds(0, lab - lp)], last_send.at[i])


def per_device(sizes, features, labels, alpha_start, order):
    ny, nz, nx, nc = sizes
    ns = nx * nc
    rows, cols = features.shape
    lab = labels.shape[1]
    lp, gp, share = lab // ny, rows // ny, cols // ns
    lam_total = reg_scale * cols * ny * nz
    n = ROUNDS + 1
    f32 = jnp.float32
    vmem = pl.BlockSpec(memory_space=pltpu.VMEM)
    dma = pltpu.SemaphoreType.DMA
    return pl.pallas_call(
        functools.partial(kernel, sizes, lam_total),
        out_shape=(jax.ShapeDtypeStruct((rows, lab), f32),) * 2,
        in_specs=[pl.BlockSpec(memory_space=pl.ANY), vmem, vmem, vmem],
        out_specs=(vmem, vmem),
        scratch_shapes=[
            pltpu.VMEM((rows, cols), jnp.bfloat16),
            pltpu.VMEM((ns * rows, share), jnp.bfloat16),
            pltpu.VMEM((n, lab, ns * rows), f32),
            pltpu.VMEM((lab, share), f32),
            pltpu.VMEM((n, lab, ns * rows), f32),
            pltpu.VMEM((n, ny * ns, lp, rows), f32),
            pltpu.VMEM((n, nz, lp, rows), f32),
            pltpu.VMEM((lab, rows), f32),
            pltpu.VMEM((lab, rows), f32),
            pltpu.VMEM((2, lab, rows), f32),
            pltpu.VMEM((rows, rows), f32),
            pltpu.VMEM((ny, gp, rows), f32),
            pltpu.VMEM((nz, gp, rows), f32),
            pltpu.VMEM((rows, rows), f32),
            dma((2,)),
            dma(()),
            dma(()),
            dma((n,)),
            dma((n,)),
            dma((n,)),
            dma((n,)),
            dma((n,)),
            dma((n,)),
            dma((3,)),
            dma((3,)),
            dma((2,)),
            dma((2,)),
        ],
        compiler_params=pltpu.CompilerParams(
            collective_id=0, has_side_effects=True, vmem_limit_bytes=48 * 1024 * 1024
        ),
        name="dual_rounds",
    )(features, labels, alpha_start, order)


def solution(mesh, grid=GRID):
    finer = Mesh(mesh.devices.reshape(grid), NAMES)
    placed = (P(SAMP, FEAT), P(SAMP, None), P(SAMP, None), P(None, SAMP))
    return jax.shard_map(
        functools.partial(per_device, grid),
        mesh=finer,
        in_specs=placed,
        out_specs=(P(SAMP, None), P(SAMP, None)),
        check_vma=False,
    )
```
